32 devices in a mesh: groups: 1, slab: 8 (over z, y), coil: 2 (over x), row: 2 (over core).
Axes of the slice: x: 2, y: 2, z: 4, core: 2. Of those that a mesh axis runs over, the one named last changes fastest.
Arguments:
- image: float32 [2, 128, 256, 128], P('groups', None, ('slab', 'row')), may hold values from -6 to 6
- sens: bfloat16 [2, 16, 128, 256, 128], P('groups', 'coil', None, ('slab', 'row')), may hold values from -1.5 to 1.5
- measured: bfloat16 [2, 16, 128, 256, 128], P('groups', 'coil', ('slab', 'row')), may hold values from -3 to 3
- mask: int32 [128, 256], P(('slab', 'row')), may hold values from 0 to 1, as said below
- thresholds: float32 [2, 7], replicated, may hold values from 0.1 to 1.5
Outputs:
- image_next: float32 [2, 128, 256, 128], P('groups', None, ('slab', 'row'))
The draws below stay inside these ranges and needn't reach their ends.
Inputs may be any that keep to these rules, and one draw needn't show every extreme that they name: `mask`: A calibration block of the 8 central phase-encode lines (ky from 60 to 67) is sampled at every kz; outside it each (ky, kz) is sampled independently at random.
All inputs are finite; a program needn't handle non-finite values.
Results may differ from the reference program's by a relative error of at most 0.013.
Values may be sent and summed in bfloat16 or wider, within the bound.
A program may use at most 128 MiB of HBM per device.

```python
import math
import jax
import jax.numpy as jnp
from jax import lax

X = 128
Y = 128
Z = 256
C = 16
LEVELS = 2


def draw_mask(key, part):
    drawn = jax.random.randint(key, (Y, Z), 0, 3)
    scattered = (drawn == 0).astype(jnp.int32)
    line_index = jnp.arange(Y, dtype=jnp.int32)[:, None]
    calibration = ((line_index >= Y // 2 - 4) & (line_index < Y // 2 + 4)).astype(jnp.int32)
    return jnp.maximum(scattered, jnp.broadcast_to(calibration, (Y, Z)))


def steps_of(key, extent, split, least, top_value):
    gain = 1.0
    for position, blocks in split:
        steps = jax.random.uniform(jax.random.fold_in(jax.random.fold_in(key, 6), position), (blocks,), jnp.float32, least / len(split), top_value / len(split))
        gain = gain * jnp.repeat(jnp.exp(steps), extent[position] // blocks).reshape((-1,) + (1,) * (len(extent) - 1 - position))
    return gain


def noise(stream_key, extent, width, bound, cuts=(), kind=jnp.bfloat16):
    result = width * jax.random.normal(stream_key, extent, jnp.float32)
    if cuts:
        result = result * steps_of(stream_key, extent, cuts, -0.22, 0.18)
    return jnp.clip(result, -bound, bound).astype(kind)


def setup_inputs(seed: int = 0, part: int = 0) -> dict:
    seeds = jax.random.split(jax.random.key(seed), 6)
    own_keys = jax.random.split(jax.random.fold_in(seeds[5], part), 6)
    image = noise(own_keys[0], (2, Y, Z, X), 1.0, 6.0, ((2, 16),), jnp.float32)
    sens = noise(own_keys[1], (2, C, Y, Z, X), 0.25, 1.5, ((1, 2), (3, 16)))
    measured = noise(own_keys[2], (2, C, Y, Z, X), 0.5, 3.0, ((1, 2), (2, 16)))
    mask = draw_mask(jax.random.fold_in(seeds[5], 71), part)
    thresholds = jnp.clip(jnp.exp(jax.random.uniform(seeds[4], (LEVELS, 7), jnp.float32, math.log(0.1), math.log(1.5))), 0.1, 1.5)
    return {"image": image, "sens": sens, "measured": measured, "mask": mask, "thresholds": thresholds}


half_root = 0.7071067811865476
quarter_root = 0.3535533905932738
step_size = 0.5

def fourier_table(length, sign):
    index = jnp.arange(length, dtype=jnp.int32)
    phase = index[:, None] * index[None, :] % length
    theta = phase.astype(jnp.float32) * jnp.float32(2.0 * math.pi / length)
    scale = jnp.float32(1.0 / math.sqrt(length))
    real = jnp.cos(theta) * scale
    imaginary = jnp.sin(theta) * (sign * scale)
    upper = jnp.stack([real, -imaginary])
    lower = jnp.stack([imaginary, real])
    return jnp.stack([upper, lower]).astype(jnp.bfloat16)

def contract(form, values, table):
    return jnp.einsum(form, values.astype(jnp.float32), table.astype(jnp.float32), precision=lax.Precision.HIGHEST)

def complex_product(left, right):
    return jnp.stack([left[0] * right[0] - left[1] * right[1], left[0] * right[1] + left[1] * right[0]])

def roll_after(values, along, offset):
    return jnp.roll(values, -offset, axis=along)

def roll_before(values, along, offset):
    return jnp.roll(values, offset, axis=along)

def split_bands(bands, along, offset, after):
    moved = after(bands, along, offset)
    return jnp.concatenate([(bands + moved) * half_root, (bands - moved) * half_root], axis=0)

def merge_bands(bands, along, offset, before):
    half = bands.shape[0] // 2
    lower = bands[:half]
    upper = bands[half:]
    return (lower + upper + before(lower - upper, along, offset)) * quarter_root

def shrink_detail(detail, limit):
    magnitude = jnp.sqrt(detail[:, 0] * detail[:, 0] + detail[:, 1] * detail[:, 1])
    limit = limit.reshape((-1, 1, 1, 1))
    factor = jnp.maximum(magnitude - limit, 0.0) / jnp.maximum(magnitude, limit)
    return detail * factor[:, None]

def wavelet_shrink(descent, thresholds, moves):
    coarse = descent[None]
    details = []
    for level in range(thresholds.shape[0]):
        offset = 2 ** level
        bands = coarse
        for along, after, before in moves:
            bands = split_bands(bands, along, offset, after)
        coarse = bands[:1]
        details.append(shrink_detail(bands[1:], thresholds[level]))
    for level in reversed(range(thresholds.shape[0])):
        offset = 2 ** level
        bands = jnp.concatenate([coarse, details[level]], axis=0)
        for along, after, before in reversed(moves):
            bands = merge_bands(bands, along, offset, before)
        coarse = bands
    return coarse[0]

def reference(image, sens, measured, mask, thresholds):
    table_readout = fourier_table(image.shape[3], -1.0)
    table_phase = fourier_table(image.shape[1], -1.0)
    table_depth = fourier_table(image.shape[2], -1.0)
    inverse_readout = fourier_table(image.shape[3], 1.0)
    inverse_phase = fourier_table(image.shape[1], 1.0)
    inverse_depth = fourier_table(image.shape[2], 1.0)
    sampled = mask.astype(jnp.float32)[None, :, :, None]

    def coil_step(total, pieces):
        coil_sens, coil_data = pieces
        sens_wide = coil_sens.astype(jnp.float32)
        coil_image = complex_product(sens_wide, image).astype(jnp.bfloat16)
        readout_done = contract('tyzj,stjk->syzk', coil_image, table_readout).astype(jnp.bfloat16)
        phase_done = contract('tjzx,stjk->skzx', readout_done, table_phase).astype(jnp.bfloat16)
        spectrum = contract('tyjx,stjk->sykx', phase_done, table_depth)
        residual = (sampled * (spectrum - coil_data.astype(jnp.float32))).astype(jnp.bfloat16)
        depth_back = contract('tyjx,stjk->sykx', residual, inverse_depth).astype(jnp.bfloat16)
        phase_back = contract('tjzx,stjk->skzx', depth_back, inverse_phase).astype(jnp.bfloat16)
        readout_back = contract('tyzj,stjk->syzk', phase_back, inverse_readout)
        term = jnp.stack([sens_wide[0] * readout_back[0] + sens_wide[1] * readout_back[1], sens_wide[0] * readout_back[1] - sens_wide[1] * readout_back[0]])
        return (total + term, None)
    gradient, _ = lax.scan(coil_step, jnp.zeros(image.shape, jnp.float32), (jnp.moveaxis(sens, 1, 0), jnp.moveaxis(measured, 1, 0)))
    descent = image - step_size * gradient
    moves = [(4, roll_after, roll_before), (2, roll_after, roll_before), (3, roll_after, roll_before)]
    return wavelet_shrink(descent, thresholds, moves)
```

```python
import functools
import math

import jax
import jax.numpy as jnp
from jax import lax
from jax.experimental import pallas as pl
from jax.experimental.pallas import tpu as pltpu
from jax.sharding import PartitionSpec as P

half_root = 0.7071067811865476
quarter_root = 0.3535533905932738
step_size = 0.5
CHUNKS = 2


def passed_along(block, axis, distance):
    devices = range(lax.axis_size(axis))
    route = [((i - distance) % len(devices), i) for i in devices]
    return lax.ppermute(block, axis, route)


def fourier_table(length, sign):
    index = jnp.arange(length, dtype=jnp.int32)
    phase = index[:, None] * index[None, :] % length
    theta = phase.astype(jnp.float32) * jnp.float32(2.0 * math.pi / length)
    scale = jnp.float32(1.0 / math.sqrt(length))
    real = jnp.cos(theta) * scale
    imaginary = jnp.sin(theta) * (sign * scale)
    upper = jnp.stack([real, -imaginary])
    lower = jnp.stack([imaginary, real])
    return jnp.stack([upper, lower]).astype(jnp.bfloat16)


def contract(form, values, table):
    return jnp.einsum(form, values, table, preferred_element_type=jnp.float32)


def complex_product(left, right):
    return jnp.stack(
        [left[0] * right[0] - left[1] * right[1], left[0] * right[1] + left[1] * right[0]]
    )


def split_plane(plane, offset):
    cells_y, cells_x = plane.shape
    moved = pltpu.roll(plane, cells_x - offset, 1)
    bands = []
    for part in (plane + moved, plane - moved):
        bands.append((part, pltpu.roll(part, cells_y - offset, 0)))
    (low, low_moved), (high, high_moved) = bands
    return [low + low_moved, high + high_moved, low - low_moved, high - high_moved]


def merge_plane(bands, offset):
    across = []
    for lower, upper in ((bands[0], bands[2]), (bands[1], bands[3])):
        across.append(lower + upper + pltpu.roll(lower - upper, offset, 0))
    lower, upper = across
    return lower + upper + pltpu.roll(lower - upper, offset, 1)


def shrink_pair(real, imaginary, limit):
    factor = jnp.maximum(1.0 - limit * lax.rsqrt(real * real + imaginary * imaginary), 0.0)
    return real * factor, imaginary * factor


def wavelet_kernel(levels, planes, limits, source, result, *scratch):
    halo = 2**levels - 1
    stop = halo + planes
    coarse_refs = (source,) + scratch[: levels - 1]
    merged_refs = (None,) + scratch[levels - 1 : 2 * (levels - 1)]
    split_ref, carry_ref = scratch[2 * (levels - 1) :]
    extent = planes + 2 * halo
    for level in range(levels - 1):
        offset = 2**level
        extent -= offset
        finer, coarser = coarse_refs[level], coarse_refs[level + 1]

        def coarsen(n, _, offset=offset, finer=finer, coarser=coarser):
            for t in range(2):
                total = finer[t, n] + finer[t, n + offset]
                total = total + pltpu.roll(total, total.shape[1] - offset, 1)
                total = total + pltpu.roll(total, total.shape[0] - offset, 0)
                coarser[t, n] = total * half_root**3
            return 0

        lax.fori_loop(0, extent, coarsen, 0)
    for level in reversed(range(levels)):
        offset = 2**level
        slots = offset + 1
        first = halo - (offset - 1)
        start = first - offset
        coarse = coarse_refs[level]

        def enter(n, _, offset=offset, coarse=coarse, slots=slots):
            for t in range(2):
                for b, band in enumerate(split_plane(coarse[t, n] * half_root**3, offset)):
                    split_ref[lax.rem(n, slots), b, t] = band
            return 0

        lax.fori_loop(start, start + offset, enter, 0)

        def advance(n, _, level=level, offset=offset, slots=slots, first=first, enter=enter):
            enter(n + offset, 0)
            here, there, back = lax.rem(n, slots), lax.rem(n + offset, slots), lax.rem(n, offset)
            merged = [[], []]
            for b in range(4):
                near = [split_ref[here, b, t] for t in range(2)]
                far = [split_ref[there, b, t] for t in range(2)]
                high = shrink_pair(near[0] - far[0], near[1] - far[1], limits[level, b + 3])
                if b:
                    low = shrink_pair(near[0] + far[0], near[1] + far[1], limits[level, b - 1])
                elif level < levels - 1:
                    low = [merged_refs[level + 1][t, n] for t in range(2)]
                else:
                    low = (near[0] + far[0], near[1] + far[1])
                for t in range(2):
                    merged[t].append(low[t] + high[t] + carry_ref[back, b, t])
                    carry_ref[back, b, t] = low[t] - high[t]

            @pl.when(n >= first)
            def _():
                for t in range(2):
                    value = merge_plane(merged[t], offset) * quarter_root**3
                    if level:
                        merged_refs[level][t, n] = value
                    else:
                        result[t, n - halo] = value

            return 0

        lax.fori_loop(start, stop, advance, 0)


def wavelet_shrink(descent, thresholds):
    levels = thresholds.shape[0]
    halo = 2**levels - 1
    parts, planes, cells_y, cells_x = descent.shape
    ends = descent[:, planes - halo :].astype(jnp.bfloat16)
    starts = descent[:, :halo].astype(jnp.bfloat16)
    before = passed_along(ends, ("slab", "row"), 1).astype(jnp.float32)
    after = passed_along(starts, ("slab", "row"), -1).astype(jnp.float32)
    source = jnp.concatenate([before, descent, after], axis=1)
    plane = (cells_y, cells_x)
    store = [pltpu.VMEM((parts, planes + 2 * halo) + plane, jnp.float32)] * (2 * (levels - 1))
    whole = pl.BlockSpec(memory_space=pltpu.VMEM)
    return pl.pallas_call(
        functools.partial(wavelet_kernel, levels, planes),
        out_shape=jax.ShapeDtypeStruct(descent.shape, jnp.float32),
        in_specs=[pl.BlockSpec(memory_space=pltpu.SMEM), whole],
        out_specs=whole,
        scratch_shapes=store
        + [
            pltpu.VMEM((2 ** (levels - 1) + 1, 4, parts) + plane, jnp.float32),
            pltpu.VMEM((2 ** (levels - 1), 4, parts) + plane, jnp.float32),
        ],
        compiler_params=pltpu.CompilerParams(vmem_limit_bytes=32 * 2**20),
        cost_estimate=pl.CostEstimate(flops=descent.size * 400, bytes_accessed=descent.size * 8, transcendentals=0),
    )(thresholds, source)


def coil_sum(partial_value):
    total = partial_value.astype(jnp.float32)
    for distance in range(1, lax.axis_size("coil")):
        total = total + passed_along(partial_value, "coil", distance).astype(jnp.float32)
    return total


def shrinkage_step(image, sens, measured, mask, thresholds):
    shards = lax.axis_size(("slab", "row"))
    readout_cells = image.shape[3]
    phase_cells = image.shape[1]
    depth_cells = measured.shape[3]
    coils = sens.shape[1]
    table_readout = fourier_table(readout_cells, -1.0)
    inverse_readout = fourier_table(readout_cells, 1.0)
    table_phase = fourier_table(phase_cells, -1.0)
    inverse_phase = fourier_table(phase_cells, 1.0)
    table_depth = fourier_table(depth_cells, -1.0)
    inverse_depth = fourier_table(depth_cells, 1.0)
    lines = phase_cells // shards
    planes = depth_cells // shards
    phase_out = table_phase.reshape(2, 2, phase_cells, shards, lines)
    phase_in = inverse_phase.reshape(2, 2, shards, lines, phase_cells)
    depth_in = table_depth.reshape(2, 2, shards, planes, depth_cells)
    depth_out = inverse_depth.reshape(2, 2, depth_cells, shards, planes)
    sampled = mask.astype(jnp.float32)[None, None, :, :, None]
    width = max(coils // CHUNKS, 1)
    exchange = functools.partial(
        lax.all_to_all, axis_name=("slab", "row"), split_axis=0, concat_axis=0, tiled=True
    )
    gradient = jnp.zeros((2, phase_cells, planes, readout_cells), jnp.float32)
    previous = None
    for first in range(0, coils, width):
        part = slice(first, first + width)
        sens_part, image_part = sens[:, part], image
        if previous is not None:
            sens_part, image_part, _ = lax.optimization_barrier((sens_part, image, previous))
        sens_wide = sens_part.astype(jnp.float32)
        coil_image = complex_product(sens_wide, image_part[:, None]).astype(jnp.bfloat16)
        readout_done = contract("tcyzj,stjk->scyzk", coil_image, table_readout).astype(jnp.bfloat16)
        phase_done = contract("tcjzx,stjdk->dsckzx", readout_done, phase_out).astype(jnp.bfloat16)
        previous = phase_done
        spread = exchange(phase_done)
        spectrum = contract("dtcyjx,stdjk->scykx", spread, depth_in)
        residual = (sampled * (spectrum - measured[:, part].astype(jnp.float32))).astype(jnp.bfloat16)
        depth_back = contract("tcyjx,stjdk->dscykx", residual, depth_out).astype(jnp.bfloat16)
        gathered = exchange(depth_back)
        phase_back = contract("dtcjzx,stdjk->sckzx", gathered, phase_in).astype(jnp.bfloat16)
        readout_back = contract("tcyzj,stjk->scyzk", phase_back, inverse_readout)
        gradient = gradient + jnp.stack(
            [
                jnp.sum(sens_wide[0] * readout_back[0] + sens_wide[1] * readout_back[1], axis=0),
                jnp.sum(sens_wide[0] * readout_back[1] - sens_wide[1] * readout_back[0], axis=0),
            ]
        )
    turned = jnp.swapaxes(gradient.astype(jnp.bfloat16), 1, 2)
    descent = jnp.swapaxes(image, 1, 2) - step_size * coil_sum(turned)
    return jnp.swapaxes(wavelet_shrink(descent, thresholds), 1, 2)


def solution(mesh):
    return jax.shard_map(
        shrinkage_step,
        mesh=mesh,
        in_specs=(
            P("groups", None, ("slab", "row"), None),
            P("groups", "coil", None, ("slab", "row"), None),
            P("groups", "coil", ("slab", "row"), None, None),
            P(("slab", "row"), None),
            P(),
        ),
        out_specs=P("groups", None, ("slab", "row"), None),
        check_vma=False,
    )
```
